32 devices in a mesh: grp: 2 (over y), leaf: 4 (over z), sub: 4 (over x, core).
Axes of the slice: x: 2, y: 2, z: 4, core: 2. Of those that a mesh axis runs over, the one named last changes fastest.
Arguments:
- targets: bfloat16 [64, 65536], P(None, ('grp', 'leaf', 'sub')), parts along dimension 1, may hold values from -6 to 6
- tree_order: int32 [32, 2048], P(('grp', 'leaf', 'sub')), parts along dimension 0, may hold values from 0 to 2047, each once within a row
- leaf_inverse: bfloat16 [128, 512, 512], P(('grp', 'leaf', 'sub')), parts along dimension 0, as said below
- cluster_basis: bfloat16 [6, 32, 65536], P(None, None, ('grp', 'leaf', 'sub')), parts along dimension 2, may hold values from -1.5 to 1.5
- coupling: float32 [32, 6, 32, 64], P(('grp', 'leaf', 'sub')), parts along dimension 0, may hold values from -0.75 to 0.75
- train_coords: bfloat16 [3, 65536], P(None, ('grp', 'leaf', 'sub')), parts along dimension 1, may hold values from 0 to 1
- test_coords: bfloat16 [3, 65536], P(None, ('grp', 'leaf', 'sub')), parts along dimension 1, may hold values from 0 to 1
- test_basis: bfloat16 [4, 32, 65536], P(None, None, ('grp', 'leaf', 'sub')), parts along dimension 2, may hold values from -2.4 to 2.4
- near_leaves: int32 [32, 8], P(('grp', 'leaf', 'sub')), parts along dimension 0, may hold values from 0 to 63, as said below
Outputs:
- posterior_mean: bfloat16 [64, 65536], P(None, ('grp', 'leaf', 'sub')), parts along dimension 1
The draws below stay inside these ranges and needn't reach their ends.
There are 2 independent parts, one for each index of `grp`. The reference program is written for one: setup_inputs(seed, part) draws one part's arguments, and reference() takes and returns one part's arrays. A program takes and returns all parts, laid end to end along the dimension named above; each array names one. Nothing has to cross between parts.
Inputs may be any that keep to these rules, and one draw needn't show every extreme that they name: `tree_order`: row d is a permutation of the positions 0 to 2047 within panel d. `near_leaves`: row d names 8 different training leaves, all held by panels d - 1, d or d + 1. `leaf_inverse`: each block is the identity plus dense full-rank entries of spread 0.5 / sqrt(512).
All inputs are finite; a program needn't handle non-finite values.
Results may differ from the reference program's by a relative error of at most 0.0035.
Values may be sent and summed in bfloat16 or wider, within the bound.
A program may use at most 64 MiB of HBM per device.

```python
import math
import jax
import jax.numpy as jnp
from jax import lax

RHS = 64
LEAF = 512
RANK = 32
NEAR = 8
LEAF_DEV = 4
TEST_DEV = 2048
GROUP_DEVS = 16
PTS_DEV = 2048
NTRAIN = 32768
LEAVES = 64
NTEST = 32768
LOCAL_LEVELS = 2
DEV_LEVELS = 4
LEVELS = 6


def draw_leaf_inverse(key, part):
    noise = jax.random.normal(jax.random.fold_in(key, 11), (LEAVES, LEAF, LEAF), jnp.float32)
    identity = jnp.eye(LEAF, dtype=jnp.float32)[None]
    return (identity + noise * (0.5 / math.sqrt(LEAF))).astype(jnp.bfloat16)


def draw_test_basis(key, part):
    levels = jnp.arange(DEV_LEVELS, dtype=jnp.float32)
    spread = 0.05 * 8.0 ** (levels / (DEV_LEVELS - 1))
    noise = jnp.clip(jax.random.normal(jax.random.fold_in(key, 23), (DEV_LEVELS, RANK, NTEST), jnp.float32), -6.0, 6.0)
    return (noise * spread[:, None, None]).astype(jnp.bfloat16)


def draw_near_leaves(key, part):
    window = 3 * LEAF_DEV
    device_ids = jnp.arange(GROUP_DEVS, dtype=jnp.int32)[:, None]
    candidates = jnp.arange(window, dtype=jnp.int32)[None, :]
    leaf_ids = (device_ids - 1) * LEAF_DEV + candidates
    valid = (leaf_ids >= 0) & (leaf_ids < LEAVES)
    scores = jax.random.randint(jax.random.fold_in(key, 7), (GROUP_DEVS, window), 0, 1 << 20, dtype=jnp.int32) * window + candidates
    scores = jnp.where(valid, scores, -1)
    chosen = lax.top_k(scores, NEAR)[1].astype(jnp.int32)
    return jnp.take_along_axis(leaf_ids, chosen, axis=1).astype(jnp.int32)


def level_of(key, shape, split, low, high):
    factor_of = 1.0
    for position, blocks in split:
        heights = jax.random.uniform(jax.random.fold_in(jax.random.fold_in(key, 6), position), (blocks,), jnp.float32, low / len(split), high / len(split))
        factor_of = factor_of * jnp.repeat(jnp.exp(heights), shape[position] // blocks).reshape((-1,) + (1,) * (len(shape) - 1 - position))
    return factor_of


def scatter_about(rng, extent, deviation, most, cuts=(), kind=jnp.bfloat16):
    entries = jax.random.normal(rng, extent, jnp.float32) * deviation
    if len(cuts) > 0:
        entries = level_of(rng, extent, cuts, -0.22, 0.18) * entries
    return jnp.clip(entries, min=-most, max=most).astype(kind)


def setup_inputs(seed: int = 0, part: int = 0) -> dict:
    key_of = jax.random.split(jax.random.key(seed), 10)
    part_splits = jax.random.split(jax.random.fold_in(key_of[9], part), 10)
    return {
        "targets": scatter_about(part_splits[0], (RHS, NTRAIN), 1.0, 6.0, ((1, 16),)),
        "tree_order": jax.vmap(lambda own: jax.random.permutation(own, PTS_DEV))(jax.random.split(part_splits[1], GROUP_DEVS)).reshape((GROUP_DEVS, PTS_DEV)).astype(jnp.int32),
        "leaf_inverse": draw_leaf_inverse(jax.random.fold_in(jax.random.fold_in(key_of[9], part), 71), part),
        "cluster_basis": scatter_about(part_splits[3], (LEVELS, RANK, NTRAIN), 0.25, 1.5, ((2, 16),)),
        "coupling": scatter_about(part_splits[4], (GROUP_DEVS, LEVELS, RANK, 2 * RANK), (2 * RANK) ** -0.5, 0.75, ((0, 16),), jnp.float32),
        "train_coords": jnp.clip(1.0 * jax.random.uniform(part_splits[5], (3, NTRAIN), jnp.float32) ** level_of(part_splits[5], (3, NTRAIN), ((1, 16),), -0.2, 0.2), 0.0, 1.0).astype(jnp.bfloat16),
        "test_coords": jnp.clip(1.0 * jax.random.uniform(part_splits[6], (3, NTEST), jnp.float32) ** level_of(part_splits[6], (3, NTEST), ((1, 16),), -0.2, 0.2), 0.0, 1.0).astype(jnp.bfloat16),
        "test_basis": draw_test_basis(jax.random.fold_in(jax.random.fold_in(key_of[9], part), 71), part),
        "near_leaves": draw_near_leaves(jax.random.fold_in(jax.random.fold_in(key_of[9], part), 71), part),
    }


variance = 2.0
length_scale = 0.5
highest = lax.Precision.HIGHEST

def matern(train_pos, test_pos):
    train_f32 = train_pos.astype(jnp.float32)
    test_f32 = test_pos.astype(jnp.float32)
    squared = jnp.zeros((train_f32.shape[1], test_f32.shape[1]), jnp.float32)
    for axis_number in range(3):
        offset = train_f32[axis_number][:, None] - test_f32[axis_number][None, :]
        squared = squared + offset * offset
    scaled = jnp.sqrt(3.0 * squared) / length_scale
    return (variance * (1.0 + scaled) * jnp.exp(-scaled)).astype(jnp.bfloat16)

def reference(targets, tree_order, leaf_inverse, cluster_basis, coupling, train_coords, test_coords, test_basis, near_leaves):
    device_base = (jnp.arange(GROUP_DEVS, dtype=jnp.int32) * PTS_DEV)[:, None]
    flat_index = (tree_order + device_base).reshape(-1).astype(jnp.int32)
    reordered = jnp.take(targets, flat_index, axis=1)

    def solve_panel(pair):
        inverse_part, target_part = pair
        return jnp.einsum('jpq,rjq->rjp', inverse_part.astype(jnp.float32), target_part.astype(jnp.float32), precision=highest)
    inverse_groups = leaf_inverse.reshape(GROUP_DEVS, LEAF_DEV, LEAF, LEAF)
    target_groups = reordered.reshape(RHS, GROUP_DEVS, LEAF_DEV, LEAF).transpose(1, 0, 2, 3)
    solved = lax.map(solve_panel, (inverse_groups, target_groups))
    state = solved.transpose(1, 0, 2, 3).reshape(RHS, NTRAIN)
    for level_index in range(LEVELS):
        child = LEAF * 2 ** level_index
        child_count = NTRAIN // child
        unit = min(child, PTS_DEV)
        unit_count = NTRAIN // unit
        level_basis = cluster_basis[level_index].astype(jnp.float32)
        coefficient = jnp.einsum('kcp,rcp->ckr', level_basis.reshape(RANK, child_count, child), state.reshape(RHS, child_count, child), precision=highest) / math.sqrt(child)
        paired = coefficient.reshape(child_count // 2, 2, RANK, RHS)
        sibling = paired[:, ::-1].reshape(child_count, RANK, RHS)
        joined = jnp.concatenate([coefficient, sibling], axis=1)
        per_unit = jnp.repeat(joined, child // unit, axis=0)
        unit_coupling = jnp.repeat(coupling[:, level_index], PTS_DEV // unit, axis=0)
        mixed = jnp.einsum('uks,usr->ukr', unit_coupling, per_unit, precision=highest)
        update = jnp.einsum('ukr,kup->rup', mixed, level_basis.reshape(RANK, unit_count, unit), precision=highest)
        state = (state.reshape(RHS, unit_count, unit) - update).reshape(RHS, NTRAIN)
    weights = state.astype(jnp.bfloat16)
    weight_leaves = weights.reshape(RHS, LEAVES, LEAF)
    coord_leaves = train_coords.reshape(3, LEAVES, LEAF)
    test_groups = test_coords.reshape(3, GROUP_DEVS, TEST_DEV).transpose(1, 0, 2)

    def near_panel(pair):
        leaf_ids, test_pos = pair
        total = jnp.zeros((RHS, TEST_DEV), jnp.float32)
        for slot_index in range(NEAR):
            leaf_id = leaf_ids[slot_index].astype(jnp.int32)
            train_pos = lax.dynamic_index_in_dim(coord_leaves, leaf_id, 1, keepdims=False)
            leaf_weights = lax.dynamic_index_in_dim(weight_leaves, leaf_id, 1, keepdims=False)
            kernel = matern(train_pos, test_pos)
            total = total + jnp.dot(leaf_weights, kernel, preferred_element_type=jnp.float32)
        return total
    near_sum = lax.map(near_panel, (near_leaves, test_groups))
    far = jnp.zeros((RHS, GROUP_DEVS, TEST_DEV), jnp.float32)
    test_levels = test_basis.reshape(DEV_LEVELS, RANK, GROUP_DEVS, TEST_DEV)
    panel_weights = weights.reshape(RHS, GROUP_DEVS, PTS_DEV).astype(jnp.float32)
    for level_index in range(DEV_LEVELS):
        span = 2 ** level_index
        level_basis = cluster_basis[LOCAL_LEVELS + level_index].reshape(RANK, GROUP_DEVS, PTS_DEV).astype(jnp.float32)
        terms = jnp.einsum('kdp,rdp->dkr', level_basis, panel_weights, precision=highest) / math.sqrt(PTS_DEV * span)
        subtree = terms.reshape(GROUP_DEVS // span, span, RANK, RHS).sum(axis=1)
        sibling_ids = (jnp.arange(GROUP_DEVS, dtype=jnp.int32) // span ^ 1).astype(jnp.int32)
        sibling = jnp.take(subtree, sibling_ids, axis=0)
        far = far + jnp.einsum('dkr,kdt->rdt', sibling, test_levels[level_index].astype(jnp.float32), precision=highest)
    mean = near_sum.transpose(1, 0, 2) / math.sqrt(NEAR * LEAF) + far
    return mean.reshape(RHS, NTEST).astype(jnp.bfloat16)
```

```python
import functools
import math

import jax
import jax.numpy as jnp
from jax import lax
from jax.experimental import pallas as pl
from jax.experimental.pallas import tpu as pltpu
from jax.sharding import PartitionSpec as P

variance = 2.0
length_scale = 0.5
highest = lax.Precision.HIGHEST
f32 = jnp.float32
bf16 = jnp.bfloat16
CHUNK = 256
TILE = 1024
FEATS = 16


def nt(a, b):
    return lax.dot_general(a, b, (((1,), (1,)), ((), ())), preferred_element_type=f32)


def tn(a, b):
    return lax.dot_general(a, b, (((0,), (0,)), ((), ())), preferred_element_type=f32)


def exact(a, b):
    return lax.dot_general(
        a, b, (((1,), (0,)), ((), ())), precision=highest, preferred_element_type=f32
    )


def halves(x):
    high = x.astype(bf16)
    return high, (x - high.astype(f32)).astype(bf16)


def thirds(x):
    first = x.astype(bf16).astype(f32)
    second = (x - first).astype(bf16).astype(f32)
    return [first, second, (x - first - second).astype(bf16).astype(f32)]


def toggled(index, mask):
    bit = 1
    while bit <= mask:
        if mask & bit:
            index = index + bit - 2 * bit * lax.rem(lax.div(index, bit), 2)
        bit *= 2
    return index


def kernel(
    panels,
    sub_size,
    order_ref,
    targets_ref,
    inverse_ref,
    basis_ref,
    coupling_ref,
    train_ref,
    test_ref,
    test_basis_ref,
    near_ref,
    out_ref,
    sent,
    received,
    far_sent,
    far_received,
    coord_window,
    features,
    test_features,
    blocks,
    weight_window,
    round_send,
    round_recv,
    far_send,
    far_recv,
    coord_send,
    coord_recv,
    weight_send,
    weight_recv,
):
    columns, points = targets_ref.shape
    leaf_count, leaf_size = inverse_ref.shape[0], inverse_ref.shape[1]
    levels, rank = basis_ref.shape[0], basis_ref.shape[1]
    near = near_ref.shape[1]
    tests = test_ref.shape[1]
    local = leaf_count.bit_length() - 1
    depth = levels - local
    me = lax.axis_index("leaf") * sub_size + lax.axis_index("sub")

    def device(index):
        return {"leaf": lax.div(index, sub_size), "sub": lax.rem(index, sub_size)}

    barrier = pltpu.get_barrier_semaphore()
    for mask in range(1, panels):
        pl.semaphore_signal(
            barrier,
            inc=1,
            device_id=device(toggled(me, mask)),
            device_id_type=pl.DeviceIdType.MESH,
        )

    scale = jnp.concatenate(
        [jnp.full((rank, 1), 1.0 / math.sqrt(leaf_size << level), f32) for level in range(levels)],
        axis=0,
    )
    basis = basis_ref[...].reshape(levels * rank, points)
    coupling = [coupling_ref[0, level] for level in range(levels)]

    stacked = jnp.concatenate(
        [targets_ref[:, h * CHUNK : (h + 1) * CHUNK] for h in range(points // CHUNK)], axis=0
    )
    order = order_ref[...]
    low, high = lax.rem(order, CHUNK), lax.div(order, CHUNK)
    solved, coefs, grams, bases = [], [], [], []
    for leaf in range(leaf_count):
        span = slice(leaf * leaf_size, (leaf + 1) * leaf_size)
        places = lax.broadcasted_iota(jnp.int32, (CHUNK, leaf_size), 0)
        chosen = jnp.where(places == low[:, span], 1.0, 0.0).astype(bf16)
        picked = jnp.dot(stacked, chosen, preferred_element_type=f32)
        taken = jnp.zeros((columns, leaf_size), f32)
        for h in range(points // CHUNK):
            taken = jnp.where(
                high[:, span] == h, picked[h * columns : (h + 1) * columns], taken
            )
        state = nt(taken.astype(bf16), inverse_ref[leaf])
        leaf_basis = basis[:, span]
        state_high, state_low = halves(state)
        coefs.append((nt(leaf_basis, state_high) + nt(leaf_basis, state_low)) * scale)
        grams.append(nt(leaf_basis, leaf_basis))
        solved.append(state)
        bases.append(leaf_basis)

    mixes = [[] for _ in range(leaf_count)]
    for level in range(local):
        rows = slice(level * rank, (level + 1) * rank)
        width = 1 << level
        child = [
            sum(coefs[c * width + i][rows] for i in range(width))
            for c in range(leaf_count // width)
        ]
        mixed = [
            exact(coupling[level], jnp.concatenate([child[c], child[c ^ 1]], axis=0))
            for c in range(leaf_count // width)
        ]
        for leaf in range(leaf_count):
            mixes[leaf].append(mixed[leaf // width])
            coefs[leaf] = coefs[leaf] - scale * exact(grams[leaf][:, rows], mixed[leaf // width])

    top = local * rank
    own = sum(coef[top:] for coef in coefs)
    gram = sum(one[top:, top:] for one in grams)
    carried = [
        scale[top + (k + 1) * rank :]
        * exact(gram[(k + 1) * rank :, k * rank : (k + 1) * rank], coupling[local + k])
        for k in range(depth - 1)
    ]

    pl.semaphore_wait(barrier, panels - 1)

    def remote(source, target, send, recv, index):
        return pltpu.make_async_remote_copy(
            src_ref=source,
            dst_ref=target,
            send_sem=send,
            recv_sem=recv,
            device_id=device(index),
            device_id_type=pl.DeviceIdType.MESH,
        )

    def shared(copy_next, copy_prev):
        def start():
            pl.when(me < panels - 1)(copy_next.start)
            pl.when(me > 0)(copy_prev.start)

        def wait():
            pl.when(me < panels - 1)(copy_next.wait_send)
            pl.when(me > 0)(copy_prev.wait_send)
            pl.when(me > 0)(copy_next.wait_recv)
            pl.when(me < panels - 1)(copy_prev.wait_recv)

        return start, wait

    after, before = lax.rem(me + 1, panels), lax.rem(me + panels - 1, panels)
    start_coords, wait_coords = shared(
        remote(train_ref, coord_window.at[0], coord_send.at[0], coord_recv.at[0], after),
        remote(train_ref, coord_window.at[1], coord_send.at[1], coord_recv.at[1], before),
    )
    start_coords()

    gain = 3.0 / (length_scale * length_scale) * math.log2(math.e) ** 2

    def norm(pos):
        return gain * (pos[0:1] * pos[0:1] + pos[1:2] * pos[1:2] + pos[2:3] * pos[2:3])

    def train_side(pos):
        ones = jnp.ones((3, points), f32)
        zero = jnp.zeros((1, points), f32)
        parts = thirds(-2.0 * gain * pos) + thirds(norm(pos)) + [ones, zero]
        return jnp.concatenate(parts, axis=0).astype(bf16)

    def put_features(panel, pos):
        made = train_side(pos.astype(f32))
        for leaf in range(leaf_count):
            features[panel * leaf_count + leaf] = made[:, leaf * leaf_size : (leaf + 1) * leaf_size]

    first_leaf = (me - 1) * leaf_count

    def window_leaf(slot):
        return jnp.clip(near_ref[0, slot] - first_leaf, 0, 3 * leaf_count - 1)

    def near_block(step, carry):
        slot, tile = lax.div(step, tests // TILE), lax.rem(step, tests // TILE)
        lanes = pl.ds(pl.multiple_of(tile * TILE, TILE), TILE)
        squared = tn(features[window_leaf(slot)], test_features[:, lanes])
        squared = jnp.maximum(squared, 1e-12)
        scaled = squared * lax.rsqrt(squared)
        value = (variance + (variance * math.log(2.0)) * scaled) * jnp.exp2(-scaled)
        blocks[pl.ds(pl.multiple_of(slot * leaf_size, leaf_size), leaf_size), lanes] = value.astype(
            bf16
        )
        return carry

    total_steps = near * (tests // TILE)
    marks = [0] + [min(16, 3 * r) for r in range(1, depth + 1)]
    cuts = [total_steps * min(m, 12) // 16 for m in marks]

    lengths = []
    for r in range(depth):
        height = (depth - r) * rank
        wide = sum((depth - 1 - k) * rank for k in range(r, depth - 1))
        lengths.append(max(height, wide))
    offsets = [sum(lengths[:r]) for r in range(depth)]

    mixed_far = []
    for r in range(depth):
        height = own.shape[0]
        rows = pl.ds(offsets[r], lengths[r])
        if carried:
            packed = jnp.concatenate(carried, axis=0)
        else:
            packed = jnp.zeros((height, 2 * rank), f32)
        wide = packed.shape[0]
        left, right = own, packed
        if height < lengths[r]:
            left = jnp.concatenate([own, jnp.zeros((lengths[r] - height, columns), f32)], axis=0)
        if wide < lengths[r]:
            right = jnp.concatenate([packed, jnp.zeros((lengths[r] - wide, 2 * rank), f32)], axis=0)
        sent[rows] = jnp.concatenate([left, right], axis=1)
        copy = remote(
            sent.at[rows], received.at[rows], round_send.at[r], round_recv.at[r], toggled(me, 1 << r)
        )
        copy.start()
        if r == 0:
            test_pos = test_ref[...].astype(f32)
            ones = jnp.ones((3, tests), f32)
            zero = jnp.zeros((1, tests), f32)
            test_features[...] = jnp.concatenate(
                [test_pos, test_pos, test_pos, ones] + thirds(norm(test_pos)) + [zero], axis=0
            ).astype(bf16)
            put_features(1, train_ref[...])
        if r == min(1, depth - 1):
            wait_coords()
            put_features(0, coord_window[0])
            put_features(2, coord_window[1])
        if r >= min(1, depth - 1):
            lax.fori_loop(cuts[r - 1] if r > 1 else 0, cuts[r], near_block, 0)
        copy.wait()
        other = received[rows]
        sibling = other[:height, :columns]
        joined = jnp.concatenate([own[:rank], sibling[:rank]], axis=0)
        mixed_far.append(exact(coupling[local + r], joined))
        if r < depth - 1:
            flipped = jnp.concatenate([sibling[:rank], own[:rank]], axis=0)
            step = (depth - 1 - r) * rank
            own = (
                own[rank:]
                + sibling[rank:]
                - exact(carried[0], joined)
                - exact(other[:step, columns:], flipped)
            )
            summed = []
            for k in range(r + 1, depth - 1):
                size = (depth - 1 - k) * rank
                summed.append(carried[k - r] + other[step : step + size, columns:])
                step += size
            carried = summed

    terms = jnp.zeros((depth * rank, columns), f32)
    for leaf in range(leaf_count):
        mix = jnp.concatenate(mixes[leaf] + mixed_far, axis=0)
        mix_high, mix_low = halves(mix)
        state = solved[leaf] - tn(mix_high, bases[leaf]) - tn(mix_low, bases[leaf])
        weights = state.astype(bf16)
        weight_window[leaf_count + leaf] = weights
        terms = terms + nt(bases[leaf][top:], weights)
    panel = weight_window.at[pl.ds(leaf_count, leaf_count)]
    start_weights, wait_weights = shared(
        remote(
            panel,
            weight_window.at[pl.ds(0, leaf_count)],
            weight_send.at[0],
            weight_recv.at[0],
            after,
        ),
        remote(
            panel,
            weight_window.at[pl.ds(2 * leaf_count, leaf_count)],
            weight_send.at[1],
            weight_recv.at[1],
            before,
        ),
    )
    start_weights()
    terms = terms * scale[top:]
    half = rank // 2
    for k in range(depth):
        far_sent[k] = jnp.concatenate(
            [terms[k * rank : k * rank + half], terms[k * rank + half : (k + 1) * rank]], axis=1
        )
    far_copies = []
    for mask in range(1, panels):
        copy = remote(
            far_sent.at[mask.bit_length() - 1],
            far_received.at[mask],
            far_send.at[mask],
            far_recv.at[mask],
            toggled(me, mask),
        )
        copy.start()
        far_copies.append(copy)
    lax.fori_loop(cuts[depth - 1] if depth > 1 else 0, total_steps, near_block, 0)
    for copy in far_copies:
        copy.wait()
    far_rows = []
    for k in range(depth):
        total = sum(far_received[mask] for mask in range(1 << k, 2 << k))
        far_rows += [total[:, :columns], total[:, columns:]]
    far_high, far_low = halves(jnp.concatenate(far_rows, axis=0))
    test_basis = test_basis_ref[...].reshape(depth * rank, tests)
    wait_weights()
    held = jnp.concatenate(
        [weight_window[window_leaf(slot)] for slot in range(near)], axis=1
    )
    for tile in range(tests // TILE):
        lanes = slice(tile * TILE, (tile + 1) * TILE)
        near_sum = jnp.dot(held, blocks[:, lanes], preferred_element_type=f32)
        far_sum = tn(far_high, test_basis[:, lanes]) + tn(far_low, test_basis[:, lanes])
        out_ref[:, lanes] = (near_sum * (1.0 / math.sqrt(near * leaf_size)) + far_sum).astype(bf16)


def shards(
    panels,
    sub_size,
    targets,
    tree_order,
    leaf_inverse,
    cluster_basis,
    coupling,
    train_coords,
    test_coords,
    test_basis,
    near_leaves,
):
    columns, points = targets.shape
    leaf_count, leaf_size = leaf_inverse.shape[0], leaf_inverse.shape[1]
    levels, rank = cluster_basis.shape[0], cluster_basis.shape[1]
    near = near_leaves.shape[1]
    tests = test_coords.shape[1]
    depth = levels - (leaf_count.bit_length() - 1)
    rows = 0
    for r in range(depth):
        wide = sum((depth - 1 - k) * rank for k in range(r, depth - 1))
        rows += max((depth - r) * rank, wide)
    vmem = pl.BlockSpec(memory_space=pltpu.VMEM)
    smem = pl.BlockSpec(memory_space=pltpu.SMEM)
    sems = pltpu.SemaphoreType.DMA
    return pl.pallas_call(
        functools.partial(kernel, panels, sub_size),
        out_shape=jax.ShapeDtypeStruct((columns, tests), bf16),
        in_specs=[vmem] * 8 + [smem],
        out_specs=vmem,
        scratch_shapes=[
            pltpu.VMEM((rows, columns + 2 * rank), f32),
            pltpu.VMEM((rows, columns + 2 * rank), f32),
            pltpu.VMEM((depth, rank // 2, 2 * columns), f32),
            pltpu.VMEM((panels, rank // 2, 2 * columns), f32),
            pltpu.VMEM((2, 3, points), bf16),
            pltpu.VMEM((3 * leaf_count, FEATS, leaf_size), bf16),
            pltpu.VMEM((FEATS, tests), bf16),
            pltpu.VMEM((near * leaf_size, tests), bf16),
            pltpu.VMEM((3 * leaf_count, columns, leaf_size), bf16),
            sems((depth,)),
            sems((depth,)),
            sems((panels,)),
            sems((panels,)),
            sems((2,)),
            sems((2,)),
            sems((2,)),
            sems((2,)),
        ],
        compiler_params=pltpu.CompilerParams(
            collective_id=0, has_side_effects=True, vmem_limit_bytes=60 * 1024 * 1024
        ),
    )(
        tree_order,
        targets,
        leaf_inverse,
        cluster_basis,
        coupling,
        train_coords,
        test_coords,
        test_basis,
        near_leaves,
    )


def solution(mesh):
    return jax.shard_map(
        functools.partial(shards, mesh.shape["leaf"] * mesh.shape["sub"], mesh.shape["sub"]),
        mesh=mesh,
        in_specs=(
            P(None, ("grp", "leaf", "sub")),
            P(("grp", "leaf", "sub"), None),
            P(("grp", "leaf", "sub"), None, None),
            P(None, None, ("grp", "leaf", "sub")),
            P(("grp", "leaf", "sub"), None, None, None),
            P(None, ("grp", "leaf", "sub")),
            P(None, ("grp", "leaf", "sub")),
            P(None, None, ("grp", "leaf", "sub")),
            P(("grp", "leaf", "sub"), None),
        ),
        out_specs=P(None, ("grp", "leaf", "sub")),
        check_vma=False,
    )
```
